32 devices in a mesh: ctx: 8 (over z, x), tp: 4 (over y, core).
Axes of the slice: x: 2, y: 2, z: 4, core: 2. Of those that a mesh axis runs over, the one named last changes fastest.
Arguments:
- queries: bfloat16 [2048, 8192], P('ctx', 'tp'), may hold values from -8 to 8
- keys: bfloat16 [2048, 1024], P('ctx'), may hold values from -7 to 7
- values: bfloat16 [2048, 1024], P('ctx'), may hold values from -6 to 6
- out_weight: bfloat16 [8192, 4096], P('tp'), may hold values from -0.25 to 0.25
- block_order: int32 [16], P('ctx'), may hold values from 0 to 15, each once
Outputs:
- projected: bfloat16 [2048, 4096], P('ctx', 'tp')
The draws below stay inside these ranges and needn't reach their ends.
Inputs may be any that keep to these rules, and one draw needn't show every extreme that they name: `block_order`: every sequence block appears exactly once.
All inputs are finite; a program needn't handle non-finite values.
Results may differ from the reference program's by a relative error of at most 0.015.
Values may be sent and summed in bfloat16 or wider, within the bound.
A program may use at most 64 MiB of HBM per device.

```python
import math
import jax
import jax.numpy as jnp
from jax import lax

QUERY_HEADS = 64
KEY_VALUE_HEADS = 8
HEAD_SIZE = 128
DW = 4096
BLK = 128
SEQUENCE_TOKENS = 2048
NBLK = 16


def shared_vectors(key):
    key_random_keys = jax.random.fold_in(key, 11)
    key_queries = jax.random.fold_in(key, 12)
    key_collection = jnp.clip(jax.random.normal(key_random_keys, (SEQUENCE_TOKENS, KEY_VALUE_HEADS * HEAD_SIZE), jnp.float32), -6.0, 6.0)
    queryset = jnp.clip(2.5 * jax.random.normal(key_queries, (SEQUENCE_TOKENS, QUERY_HEADS * HEAD_SIZE), jnp.float32), -8.0, 8.0)
    return (key_collection.astype(jnp.bfloat16), queryset.astype(jnp.bfloat16))


def draw_queries(key, part):
    return shared_vectors(key)[1]


def draw_keys(key, part):
    return shared_vectors(key)[0]


def steps_of(key, shape, split, least, largest):
    def one(dim, parts):
        heights = jax.random.uniform(jax.random.fold_in(jax.random.fold_in(key, 6), dim), (parts,), jnp.float32, least / len(split), largest / len(split))
        return jnp.repeat(jnp.exp(heights), shape[dim] // parts).reshape((-1,) + (1,) * (len(shape) - dim - 1))

    gain = one(*split[0])
    for cut in split[1:]:
        gain = gain * one(*cut)
    return gain


def noise(key, extent, deviation, bound, cuts=(), kind=jnp.bfloat16):
    drawn = jax.random.normal(key, extent, jnp.float32) * deviation
    if len(cuts) > 0:
        drawn = steps_of(key, extent, cuts, -0.22, 0.18) * drawn
    return jnp.clip(drawn, min=-bound, max=bound).astype(kind)


def setup_inputs(seed: int = 0) -> dict:
    key_list = jax.random.split(jax.random.key(seed), 6)
    return {
        "queries": draw_queries(jax.random.fold_in(key_list[5], 71), 0),
        "keys": draw_keys(jax.random.fold_in(key_list[5], 71), 0),
        "values": noise(key_list[2], (SEQUENCE_TOKENS, KEY_VALUE_HEADS * HEAD_SIZE), 1.0, 6.0, ((0, 8),)),
        "out_weight": noise(key_list[3], (QUERY_HEADS * HEAD_SIZE, DW), (QUERY_HEADS * HEAD_SIZE // 16) ** -0.5, 0.25, ((0, 4),)),
        "block_order": jax.random.permutation(key_list[4], NBLK).astype(jnp.int32),
    }


def reference(queries, keys, values, out_weight, block_order):
    head_group = QUERY_HEADS // KEY_VALUE_HEADS
    offsets = jnp.arange(BLK, dtype=jnp.int32)
    positions = (block_order[:, None].astype(jnp.int32) * BLK + offsets[None, :]).reshape(-1)
    scale = 1.0 / math.sqrt(HEAD_SIZE)
    q_heads = jnp.transpose(queries.reshape(SEQUENCE_TOKENS, QUERY_HEADS, HEAD_SIZE), (1, 0, 2))
    key_head_rows = jnp.transpose(keys.reshape(SEQUENCE_TOKENS, KEY_VALUE_HEADS, HEAD_SIZE), (1, 0, 2))
    value_head_rows = jnp.transpose(values.reshape(SEQUENCE_TOKENS, KEY_VALUE_HEADS, HEAD_SIZE), (1, 0, 2))
    q_pos = positions.reshape(SEQUENCE_TOKENS // BLK, BLK)

    def one_head(head):
        k_rows = key_head_rows[head // head_group]
        v_rows = value_head_rows[head // head_group]
        q_blocks = q_heads[head].reshape(SEQUENCE_TOKENS // BLK, BLK, HEAD_SIZE)

        def one_block(item):
            q_rows, rows_pos = item
            scores = jnp.dot(q_rows, k_rows.T, preferred_element_type=jnp.float32) * scale
            visible = positions[None, :] <= rows_pos[:, None]
            top = lax.optimization_barrier(jnp.max(jnp.where(visible, scores, -jnp.inf), axis=1, keepdims=True))
            weights = jnp.where(visible, jnp.exp(scores - top), 0.0)
            total = lax.optimization_barrier(jnp.sum(weights, axis=1, keepdims=True))
            return jnp.dot(weights.astype(jnp.bfloat16), v_rows, preferred_element_type=jnp.float32) / total
        return lax.map(one_block, (q_blocks, q_pos)).reshape(SEQUENCE_TOKENS, HEAD_SIZE)
    heads_out = lax.map(one_head, jnp.arange(QUERY_HEADS, dtype=jnp.int32))
    attended = jnp.transpose(heads_out, (1, 0, 2)).reshape(SEQUENCE_TOKENS, QUERY_HEADS * HEAD_SIZE).astype(jnp.bfloat16)
    return jnp.dot(attended, out_weight, preferred_element_type=jnp.float32).astype(jnp.bfloat16)
```

```python
import functools
import math

import jax
import jax.numpy as jnp
from jax import lax
from jax.experimental import pallas as pl
from jax.experimental.pallas import tpu as pltpu
from jax.sharding import PartitionSpec as P

QUERY_HEADS = 64
KEY_VALUE_HEADS = 8
HEAD_SIZE = 128
MESH = pl.DeviceIdType.MESH
NT = (((1,), (1,)), ((), ()))


def kernel(dims, q_hbm, k_hbm, v_hbm, w_hbm, order, o_ref, q, w, kv, orders, mask, eye, scores,
           top, acc, pair_out, pair_in, far_out, far_in, load_sem, send, recv,
           pair_send, pair_recv, far_send, far_recv):
    n, tp, rows, heads, kv_heads, wide = dims
    line, groups = n // 2, tp // 2
    blocks = rows // 128
    per_kv = heads // kv_heads
    tile = per_kv * 128
    me, t = lax.axis_index("ctx"), lax.axis_index("tp")
    a, b = me // 2, lax.rem(me, 2)
    y, c = t // 2, lax.rem(t, 2)
    other = 1 - b
    partner = (me, y * 2 + 1 - c)

    def far(i):
        return lax.rem(y + i, groups)

    first = t * heads // (QUERY_HEADS // KEY_VALUE_HEADS)
    own = pl.ds(pl.multiple_of(me * rows, 128), rows)
    key_parts = range(0, 2 * kv_heads, 2)
    value_parts = range(1, 2 * kv_heads, 2)
    loads = {}
    for p in (*key_parts, *value_parts):
        src = v_hbm if p % 2 else k_hbm
        cols = pl.ds(pl.multiple_of((first + p // 2) * HEAD_SIZE, 128), HEAD_SIZE)
        loads[p] = pltpu.make_async_copy(src.at[:, cols], kv.at[p, own, :], load_sem.at[p])
        loads[p].start()
    q_load = pltpu.make_async_copy(q_hbm, q, load_sem.at[2 * kv_heads])
    w_load = pltpu.make_async_copy(w_hbm, w, load_sem.at[2 * kv_heads + 1])
    q_load.start()
    for i in range(blocks):
        orders[pl.ds(me, 1), i:i + 1, :] = jnp.full((1, 1, 128), order[i], jnp.int32)

    def guarded(cond, act):
        pl.when(cond)(act)

    up, down, across = a + 1 < line, a > 0, a * 2 + other

    barrier = pltpu.get_barrier_semaphore()

    def greet(target):
        pl.semaphore_signal(barrier, inc=1, device_id=target, device_id_type=MESH)

    guarded(up, lambda: greet((me + 2, t)))
    guarded(down, lambda: greet((me - 2, t)))
    greet((across, t))
    greet(partner)
    for i in range(1, groups):
        greet((me, far(i) * 2 + c))
    pl.semaphore_wait(barrier, 1 + groups + up.astype(jnp.int32) + down.astype(jnp.int32))

    marks = 2 * kv_heads

    def piece(p, block, way, target):
        at = pl.ds(pl.multiple_of(block * rows, 128), rows)
        ref = orders.at[block] if p == marks else kv.at[p, at, :]
        return pltpu.make_async_remote_copy(
            src_ref=ref, dst_ref=ref, send_sem=send.at[p, block, way],
            recv_sem=recv.at[p, block], device_id=(target, t), device_id_type=MESH)

    def send_up(p, block):
        piece(p, block, 0, me + 2).start()

    def send_down(p, block):
        piece(p, block, 1, me - 2).start()

    def send_across(p, block):
        piece(p, block, 2, across).start()

    def arrived(p, block):
        piece(p, block, 2, me).wait_recv()

    def column(i):
        near = jnp.minimum(a, line - 1 - a)
        s = (i + 1) // 2
        zigzag = jnp.where(lax.rem(i, 2) == 1, a - s, a + s)
        onward = jnp.where(a < line - 1 - a, i, line - 1 - i)
        return jnp.where(i <= 2 * near, zigzag, onward)

    def onward(p, block):
        z = block // 2
        guarded(jnp.logical_and(up, z <= a), lambda: send_up(p, block))
        guarded(jnp.logical_and(down, z >= a), lambda: send_down(p, block))

    def near(i):
        return column(i) * 2 + b

    def crossed(i):
        return column(i) * 2 + other

    row = lax.broadcasted_iota(jnp.int32, (128, 128), 0)
    col = lax.broadcasted_iota(jnp.int32, (128, 128), 1)

    def build(i):
        for j in range(blocks):
            kpos = orders[pl.ds(i, 1), j:j + 1, :][0] * 128 + row
            for g in range(blocks):
                qpos = orders[pl.ds(me, 1), g:g + 1, :][0] * 128 + col
                at = pl.ds(pl.multiple_of(i * rows + j * 128, 128), 128)
                mask[g, at, :] = jnp.where(kpos <= qpos, 0.0, -1e30).astype(jnp.bfloat16)

    for p in (marks, *key_parts):
        if p != marks:
            loads[p].wait()
        onward(p, me)
        send_across(p, me)
    for p in value_parts:
        loads[p].wait()
        onward(p, me)
    send_across(1, me)
    w_load.start()
    eye[...] = (row == col).astype(jnp.bfloat16)
    top[...] = jnp.full(top.shape, -3e38, jnp.float32)
    q_load.wait()

    factor = math.log2(math.e) / math.sqrt(HEAD_SIZE)

    def score(slot, block):
        at = pl.ds(pl.multiple_of(block * rows, 128), rows)
        e = eye[...]
        for h in range(kv_heads):
            for g in range(blocks):
                ka = jnp.concatenate([kv[2 * h, at, :], mask[g, at, :]], axis=1)
                qa = jnp.concatenate(
                    [jnp.concatenate([q[g * 128:(g + 1) * 128, m * 128:(m + 1) * 128], e], axis=1)
                     for m in range(h * per_kv, (h + 1) * per_kv)], axis=0)
                s = lax.dot_general(qa, ka, NT, preferred_element_type=jnp.float32) * factor
                to = slice((h * blocks + g) * tile, (h * blocks + g + 1) * tile)
                scores[slot, to, :] = s
                best = top[to, :]
                for j in range(0, rows, 128):
                    best = jnp.maximum(best, s[:, j:j + 128])
                top[to, :] = best

    def relay_keys(i):
        for p in (marks, *key_parts):
            arrived(p, near(i))
            onward(p, near(i))
            send_across(p, near(i))
        build(near(i))

    def relay_values(i):
        for p in value_parts:
            arrived(p, near(i))
            onward(p, near(i))
        for p in value_parts:
            send_across(p, near(i))

    def take_keys(i):
        for p in (marks, *key_parts):
            arrived(p, crossed(i))
        build(crossed(i))

    build(me)
    score(0, me)
    for i in range(1, line):
        relay_keys(i)
        if i > 1:
            relay_values(i - 1)
            score(2 * i - 3, crossed(i - 2))
        else:
            take_keys(0)
            for p in value_parts[1:]:
                send_across(p, me)
        score(2 * i, near(i))
        if i > 1:
            take_keys(i - 1)
    score(2 * line - 3, crossed(line - 2))
    relay_values(line - 1)
    take_keys(line - 1)
    score(2 * line - 1, crossed(line - 1))

    def settle(i, _):
        at = pl.ds(pl.multiple_of(i * tile, 128), tile)
        top[at, :] = jnp.broadcast_to(jnp.max(top[at, :], axis=1, keepdims=True), (tile, 128))
        return 0
    lax.fori_loop(0, kv_heads * blocks, settle, 0)
    acc[...] = jnp.zeros(acc.shape, jnp.float32)

    ones = jnp.ones((2 * rows, 128), jnp.bfloat16)

    def value_step(i, _):
        block, over = near(i), crossed(i)
        for p in value_parts:
            arrived(p, over)
        for h in range(kv_heads):
            va = jnp.concatenate([
                jnp.concatenate([kv[2 * h + 1, pl.ds(pl.multiple_of(block * rows, 128), rows), :],
                                 kv[2 * h + 1, pl.ds(pl.multiple_of(over * rows, 128), rows), :]],
                                axis=0), ones], axis=1)
            for g in range(blocks):
                to = slice((h * blocks + g) * tile, (h * blocks + g + 1) * tile)
                best = top[to, :]
                weight = jnp.concatenate(
                    [jnp.exp2(scores[2 * i + x, to, j:j + 128] - best).astype(jnp.bfloat16)
                     for x in range(2) for j in range(0, rows, 128)], axis=1)
                acc[to, :] += jnp.dot(weight, va, preferred_element_type=jnp.float32)
        return 0
    lax.fori_loop(0, line, value_step, 0)

    att = q
    for h in range(kv_heads):
        for g in range(blocks):
            for m in range(per_kv):
                at = ((h * blocks + g) * per_kv + m) * 128
                res = acc[at:at + 128, :128] / acc[at:at + 128, 128:]
                cols = (h * per_kv + m) * 128
                att[g * 128:(g + 1) * 128, cols:cols + 128] = res.astype(jnp.bfloat16)

    quarter = o_ref.shape[1]
    parts = quarter // wide
    w_load.wait()

    def product(group, core, j):
        cols = pl.ds(pl.multiple_of((group * 2 + core) * quarter + j * wide, 128), wide)
        return jnp.dot(att[...], w[:, cols], preferred_element_type=jnp.float32)

    def pair_copy(i, j):
        return pltpu.make_async_remote_copy(
            src_ref=pair_out.at[i, j], dst_ref=pair_in.at[i, j], send_sem=pair_send.at[i, j],
            recv_sem=pair_recv.at[i, j], device_id=partner, device_id_type=MESH)

    def far_copy(i, j):
        return pltpu.make_async_remote_copy(
            src_ref=far_out.at[i - 1, j], dst_ref=far_in.at[i - 1, j], send_sem=far_send.at[i, j],
            recv_sem=far_recv.at[i, j], device_id=(me, far(i) * 2 + c), device_id_type=MESH)

    def far_step(k, _):
        i, j = 1 + k // parts, lax.rem(k, parts)
        pair_out[i, j] = product(far(i), 1 - c, j).astype(jnp.bfloat16)
        pair_copy(i, j).start()
        mine = product(far(i), c, j)
        pair_copy(i, j).wait_recv()
        far_out[i - 1, j] = (mine + pair_in[i, j].astype(jnp.float32)).astype(jnp.bfloat16)
        far_copy(i, j).start()
        return 0
    lax.fori_loop(0, (groups - 1) * parts, far_step, 0)

    def near_rows(j):
        return pl.ds(pl.multiple_of(j * rows, 128), rows)

    def near_step(j, _):
        pair_out[0, j] = product(y, 1 - c, j).astype(jnp.bfloat16)
        pair_copy(0, j).start()
        acc[near_rows(j), :wide] = product(y, c, j)
        return 0
    lax.fori_loop(0, parts, near_step, 0)

    def close_step(j, _):
        pair_copy(0, j).wait_recv()
        res = acc[near_rows(j), :wide] + pair_in[0, j].astype(jnp.float32)
        for i in range(1, groups):
            far_copy(i, j).wait_recv()
            res = res + far_in[i - 1, j].astype(jnp.float32)
        o_ref[:, pl.ds(pl.multiple_of(j * wide, 128), wide)] = res.astype(jnp.bfloat16)
        return 0
    lax.fori_loop(0, parts, close_step, 0)

    def drain(i, _):
        for p in range(2 * kv_heads + 1):
            blk = i * 2 + b
            guarded(jnp.logical_and(up, i <= a), lambda: piece(p, blk, 0, me + 2).wait_send())
            guarded(jnp.logical_and(down, i >= a), lambda: piece(p, blk, 1, me - 2).wait_send())
            piece(p, blk, 2, across).wait_send()
        return 0
    lax.fori_loop(0, line, drain, 0)

    def drain_out(j, _):
        for i in range(groups):
            pair_copy(i, j).wait_send()
            if i:
                far_copy(i, j).wait_send()
        return 0
    lax.fori_loop(0, parts, drain_out, 0)


def shards(n, tp, queries, keys, values, out_weight, block_order):
    rows = queries.shape[0]
    heads = queries.shape[1] // HEAD_SIZE
    group = QUERY_HEADS // KEY_VALUE_HEADS
    kv_heads = max(1, heads // group)
    quarter = out_weight.shape[1] // tp
    wide = min(256, quarter)
    parts, groups, tokens, blocks = quarter // wide, tp // 2, n * rows, rows // 128
    dims = (n, tp, rows, heads, kv_heads, wide)
    any_space = pl.BlockSpec(memory_space=pl.ANY)
    dma = pltpu.SemaphoreType.DMA
    bf16 = jnp.bfloat16
    swap = pltpu.VMEM((groups, parts, rows, wide), bf16)
    swap_far = pltpu.VMEM((groups - 1, parts, rows, wide), bf16)
    return pl.pallas_call(
        functools.partial(kernel, dims),
        out_shape=jax.ShapeDtypeStruct((rows, quarter), bf16),
        in_specs=[any_space] * 4 + [pl.BlockSpec(memory_space=pltpu.SMEM)],
        out_specs=pl.BlockSpec(memory_space=pltpu.VMEM),
        scratch_shapes=[
            pltpu.VMEM(queries.shape, bf16),
            pltpu.VMEM(out_weight.shape, bf16),
            pltpu.VMEM((2 * kv_heads, tokens, HEAD_SIZE), bf16),
            pltpu.VMEM((n, 8, 128), jnp.int32),
            pltpu.VMEM((blocks, tokens, 128), bf16),
            pltpu.VMEM((128, 128), bf16),
            pltpu.VMEM((n, heads * rows, rows), jnp.float32),
            pltpu.VMEM((heads * rows, 128), jnp.float32),
            pltpu.VMEM((heads * rows, 256), jnp.float32),
            swap, swap, swap_far, swap_far,
            dma((2 * kv_heads + 2,)),
            dma((2 * kv_heads + 1, n, 3)), dma((2 * kv_heads + 1, n)),
            dma((groups, parts)), dma((groups, parts)), dma((groups, parts)), dma((groups, parts)),
        ],
        compiler_params=pltpu.CompilerParams(
            collective_id=0, has_side_effects=True, vmem_limit_bytes=67043328),
    )(queries, keys, values, out_weight, block_order)


def solution(mesh):
    n, tp = mesh.shape["ctx"], mesh.shape["tp"]
    in_specs = (P("ctx", "tp"), P("ctx", None), P("ctx", None), P("tp", None), P("ctx"))
    return jax.shard_map(functools.partial(shards, n, tp), mesh=mesh, in_specs=in_specs,
                         out_specs=P("ctx", "tp"), check_vma=False)
```

```python
import functools
import math

import jax
import jax.numpy as jnp
from jax import lax
from jax.experimental import pallas as pl
from jax.experimental.pallas import tpu as pltpu
from jax.sharding import PartitionSpec as P

QUERY_HEADS = 64
KEY_VALUE_HEADS = 8
HEAD_SIZE = 128
MESH = pl.DeviceIdType.MESH
NT = (((1,), (1,)), ((), ()))


def kernel(dims, q_hbm, k_hbm, v_hbm, w_hbm, order, o_ref, q, w, kv, orders, mask, eye, scores,
           top, acc, pair_out, pair_in, far_out, far_in, load_sem, send, recv,
           pair_send, pair_recv, far_send, far_recv):
    n, tp, rows, heads, kv_heads, wide = dims
    line, groups = n // 2, tp // 2
    blocks = rows // 128
    per_kv = heads // kv_heads
    tile = per_kv * 128
    me, t = lax.axis_index("ctx"), lax.axis_index("tp")
    a, b = me // 2, lax.rem(me, 2)
    y, c = t // 2, lax.rem(t, 2)
    other = 1 - b
    partner = (me, y * 2 + 1 - c)

    def far(i):
        return lax.rem(y + i, groups)

    first = t * heads // (QUERY_HEADS // KEY_VALUE_HEADS)
    own = pl.ds(pl.multiple_of(me * rows, 128), rows)
    key_parts = range(0, 2 * kv_heads, 2)
    value_parts = range(1, 2 * kv_heads, 2)
    loads = {}
    for p in (*key_parts, *value_parts):
        src = v_hbm if p % 2 else k_hbm
        cols = pl.ds(pl.multiple_of((first + p // 2) * HEAD_SIZE, 128), HEAD_SIZE)
        loads[p] = pltpu.make_async_copy(src.at[:, cols], kv.at[p, own, :], load_sem.at[p])
        loads[p].start()
    q_load = pltpu.make_async_copy(q_hbm, q, load_sem.at[2 * kv_heads])
    w_load = pltpu.make_async_copy(w_hbm, w, load_sem.at[2 * kv_heads + 1])
    q_load.start()
    for i in range(blocks):
        orders[pl.ds(me, 1), i:i + 1, :] = jnp.full((1, 1, 128), order[i], jnp.int32)

    def guarded(cond, act):
        pl.when(cond)(act)

    up, down, across = a + 1 < line, a > 0, a * 2 + other

    barrier = pltpu.get_barrier_semaphore()

    def greet(target):
        pl.semaphore_signal(barrier, inc=1, device_id=target, device_id_type=MESH)

    guarded(up, lambda: greet((me + 2, t)))
    guarded(down, lambda: greet((me - 2, t)))
    greet((across, t))
    greet(partner)
    for i in range(1, groups):
        greet((me, far(i) * 2 + c))
    pl.semaphore_wait(barrier, 1 + groups + up.astype(jnp.int32) + down.astype(jnp.int32))

    marks = 2 * kv_heads

    def piece(p, block, way, target):
        at = pl.ds(pl.multiple_of(block * rows, 128), rows)
        ref = orders.at[block] if p == marks else kv.at[p, at, :]
        return pltpu.make_async_remote_copy(
            src_ref=ref, dst_ref=ref, send_sem=send.at[p, block, way],
            recv_sem=recv.at[p, block], device_id=(target, t), device_id_type=MESH)

    def send_up(p, block):
        piece(p, block, 0, me + 2).start()

    def send_down(p, block):
        piece(p, block, 1, me - 2).start()

    def send_across(p, block):
        piece(p, block, 2, across).start()

    def arrived(p, block):
        piece(p, block, 2, me).wait_recv()

    def column(i):
        near = jnp.minimum(a, line - 1 - a)
        s = (i + 1) // 2
        zigzag = jnp.where(lax.rem(i, 2) == 1, a - s, a + s)
        onward = jnp.where(a < line - 1 - a, i, line - 1 - i)
        return jnp.where(i <= 2 * near, zigzag, onward)

    def onward(p, block):
        z = block // 2
        guarded(jnp.logical_and(up, z <= a), lambda: send_up(p, block))
        guarded(jnp.logical_and(down, z >= a), lambda: send_down(p, block))

    def near(i):
        return column(i) * 2 + b

    def crossed(i):
        return column(i) * 2 + other

    row = lax.broadcasted_iota(jnp.int32, (128, 128), 0)
    col = lax.broadcasted_iota(jnp.int32, (128, 128), 1)

    def build(i):
        for j in range(blocks):
            kpos = orders[pl.ds(i, 1), j:j + 1, :][0] * 128 + row
            for g in range(blocks):
                qpos = orders[pl.ds(me, 1), g:g + 1, :][0] * 128 + col
                at = pl.ds(pl.multiple_of(i * rows + j * 128, 128), 128)
                mask[g, at, :] = jnp.where(kpos <= qpos, 0.0, -1e30).astype(jnp.bfloat16)

    for p in (marks, *key_parts):
        if p != marks:
            loads[p].wait()
        onward(p, me)
        send_across(p, me)
    for p in value_parts:
        loads[p].wait()
        onward(p, me)
    send_across(1, me)
    w_load.start()
    eye[...] = (row == col).astype(jnp.bfloat16)
    q_load.wait()

    factor = math.log2(math.e) / math.sqrt(HEAD_SIZE)

    half = line // 2

    last = line - 1

    def near_slot(i):
        return 2 * i if i < last else 0

    def crossed_slot(i):
        return 2 * i + 1 if i < last - 1 else i - last + 2

    def span(h, g):
        return slice((h * blocks + g) * tile, (h * blocks + g + 1) * tile)

    def score(place, block, side, fresh=False):
        at = pl.ds(pl.multiple_of(block * rows, 128), rows)
        e = eye[...]
        for h in range(kv_heads):
            for g in range(blocks):
                ka = jnp.concatenate([kv[2 * h, at, :], mask[g, at, :]], axis=1)
                qa = jnp.concatenate(
                    [jnp.concatenate([q[g * 128:(g + 1) * 128, m * 128:(m + 1) * 128], e], axis=1)
                     for m in range(h * per_kv, (h + 1) * per_kv)], axis=0)
                s = lax.dot_general(qa, ka, NT, preferred_element_type=jnp.float32) * factor
                to = span(h, g)
                scores[place, to, :] = s
                best = None if fresh else top[side, to, :]
                for j in range(0, rows, 128):
                    best = s[:, j:j + 128] if best is None else jnp.maximum(best, s[:, j:j + 128])
                top[side, to, :] = best

    def score_near(i):
        score(near_slot(i), near(i), i // half, i % half == 0)

    def score_crossed(i):
        score(crossed_slot(i), crossed(i), i // half)

    def relay_keys(i):
        for p in (marks, *key_parts):
            arrived(p, near(i))
            onward(p, near(i))
            send_across(p, near(i))
        build(near(i))

    def relay_values(i):
        for p in value_parts:
            arrived(p, near(i))
            onward(p, near(i))

    def cross_values(i):
        for p in value_parts:
            send_across(p, near(i))

    def take_keys(i):
        for p in (marks, *key_parts):
            arrived(p, crossed(i))
        build(crossed(i))

    def take_values(i):
        for p in value_parts:
            arrived(p, crossed(i))

    def peak(side, at):
        return jnp.broadcast_to(jnp.max(top[side, at, :], axis=1, keepdims=True), (tile, 128))

    def settle_first():
        def body(i, _):
            at = pl.ds(pl.multiple_of(i * tile, 128), tile)
            top[0, at, :] = peak(0, at)
            return 0
        lax.fori_loop(0, kv_heads * blocks, body, 0)

    def settle_second():
        def body(i, _):
            at = pl.ds(pl.multiple_of(i * tile, 128), tile)
            before = top[0, at, :]
            after = jnp.maximum(before, peak(1, at))
            top[1, at, :] = after
            shrink = jnp.exp2(before - after)
            acc[at, :] = acc[at, :] * jnp.concatenate([shrink, shrink], axis=1)
            return 0
        lax.fori_loop(0, kv_heads * blocks, body, 0)

    def summed(h, g, pieces, side):
        to = span(h, g)
        best = top[side, to, :]
        weight = jnp.concatenate(
            [jnp.exp2(scores[place, to, j:j + 128] - best).astype(jnp.bfloat16)
             for place, _ in pieces for j in range(0, rows, 128)], axis=1)
        va = jnp.concatenate([kv[2 * h + 1, pl.ds(pl.multiple_of(block * rows, 128), rows), :]
                              for _, block in pieces], axis=0)
        va = jnp.concatenate([va, jnp.ones(va.shape, jnp.bfloat16)], axis=1)
        return jnp.dot(weight, va, preferred_element_type=jnp.float32)

    def absorb(pieces, side, fresh=False):
        for h in range(kv_heads):
            for g in range(blocks):
                part = summed(h, g, pieces, side)
                acc[span(h, g), :] = part if fresh else acc[span(h, g), :] + part

    def absorb_pair(i):
        absorb([(near_slot(i), near(i)), (crossed_slot(i), crossed(i))], i // half, i == 0)

    build(me)
    score_near(0)
    relay_keys(1)
    take_keys(0)
    for p in value_parts[1:]:
        send_across(p, me)
    score_near(1)
    for i in range(2, line - 1):
        relay_keys(i)
        if i == 2:
            score_crossed(0)
            relay_values(1)
        cross_values(i - 1)
        relay_values(i)
        score_near(i)
        take_keys(i - 1)
        score_crossed(i - 1)
    relay_keys(last)
    for i in range(half - 1):
        take_values(i)
    settle_first()
    cross_values(last - 1)
    for i in range(half - 1):
        absorb_pair(i)
    take_keys(last - 1)
    score_near(last)
    relay_values(last)
    score_crossed(last - 1)
    cross_values(last)
    take_values(half - 1)
    absorb_pair(half - 1)
    take_keys(last)
    score_crossed(last)
    settle_second()
    for i in range(half, last):
        take_values(i)
        absorb_pair(i)
    absorb([(near_slot(last), near(last))], 1)

    att = q

    def finish(g):
        for h in range(kv_heads):
            whole = acc[span(h, g), :] + summed(h, g, [(crossed_slot(last), crossed(last))], 1)
            res = (whole[:, :128] / whole[:, 128:]).astype(jnp.bfloat16)
            for m in range(per_kv):
                cols = (h * per_kv + m) * 128
                att[g * 128:(g + 1) * 128, cols:cols + 128] = res[m * 128:(m + 1) * 128]

    quarter = o_ref.shape[1]
    parts = quarter // wide

    def product(g, group, core, j):
        cols = pl.ds(pl.multiple_of((group * 2 + core) * quarter + j * wide, 128), wide)
        at = pl.ds(pl.multiple_of(g * 128, 128), 128)
        return jnp.dot(att[at, :], w[:, cols], preferred_element_type=jnp.float32)

    def pair_copy(i, k):
        return pltpu.make_async_remote_copy(
            src_ref=pair_out.at[i, k], dst_ref=pair_in.at[i, k], send_sem=pair_send.at[i, k],
            recv_sem=pair_recv.at[i, k], device_id=partner, device_id_type=MESH)

    def far_copy(i, k):
        return pltpu.make_async_remote_copy(
            src_ref=far_out.at[i - 1, k], dst_ref=far_in.at[i - 1, k], send_sem=far_send.at[i, k],
            recv_sem=far_recv.at[i, k], device_id=(me, far(i) * 2 + c), device_id_type=MESH)

    def lend(g, i, j):
        k = g * parts + j
        pair_out[i, k] = product(g, far(i), 1 - c, j).astype(jnp.bfloat16)
        pair_copy(i, k).start()

    def ship(g, i, j):
        k = g * parts + j
        mine = product(g, far(i), c, j)
        pair_copy(i, k).wait_recv()
        far_out[i - 1, k] = (mine + pair_in[i, k].astype(jnp.float32)).astype(jnp.bfloat16)
        far_copy(i, k).start()

    take_values(last)
    trips = [(g, i, j) for g in range(blocks) for i in range(1, groups) for j in range(parts)]
    ahead = 3
    for s, trip in enumerate(trips):
        if s % (len(trips) // blocks) == 0:
            finish(trip[0])
        if s == 0:
            w_load.wait()
        lend(*trip)
        if s >= ahead:
            ship(*trips[s - ahead])
    for trip in trips[-ahead:]:
        ship(*trip)

    def spot(k):
        return pl.ds(pl.multiple_of(k * 128, 128), 128)

    def near_step(k, _):
        g, j = k // parts, lax.rem(k, parts)
        lend(g, 0, j)
        acc[spot(k), :wide] = product(g, y, c, j)
        return 0
    lax.fori_loop(0, blocks * parts, near_step, 0)

    def close_step(k, _):
        g, j = k // parts, lax.rem(k, parts)
        pair_copy(0, k).wait_recv()
        res = acc[spot(k), :wide] + pair_in[0, k].astype(jnp.float32)
        for i in range(1, groups):
            far_copy(i, k).wait_recv()
            res = res + far_in[i - 1, k].astype(jnp.float32)
        o_ref[pl.ds(pl.multiple_of(g * 128, 128), 128),
              pl.ds(pl.multiple_of(j * wide, 128), wide)] = res.astype(jnp.bfloat16)
        return 0
    lax.fori_loop(0, blocks * parts, close_step, 0)

    def drain(i, _):
        for p in range(2 * kv_heads + 1):
            blk = i * 2 + b
            guarded(jnp.logical_and(up, i <= a), lambda: piece(p, blk, 0, me + 2).wait_send())
            guarded(jnp.logical_and(down, i >= a), lambda: piece(p, blk, 1, me - 2).wait_send())
            piece(p, blk, 2, across).wait_send()
        return 0
    lax.fori_loop(0, line, drain, 0)

    def drain_out(j, _):
        for i in range(groups):
            pair_copy(i, j).wait_send()
            if i:
                far_copy(i, j).wait_send()
        return 0
    lax.fori_loop(0, blocks * parts, drain_out, 0)


def shards(n, tp, queries, keys, values, out_weight, block_order):
    rows = queries.shape[0]
    heads = queries.shape[1] // HEAD_SIZE
    group = QUERY_HEADS // KEY_VALUE_HEADS
    kv_heads = max(1, heads // group)
    quarter = out_weight.shape[1] // tp
    wide = min(256, quarter)
    parts, groups, tokens, blocks = quarter // wide, tp // 2, n * rows, rows // 128
    dims = (n, tp, rows, heads, kv_heads, wide)
    hbm_space = pl.BlockSpec(memory_space=pltpu.HBM)
    dma = pltpu.SemaphoreType.DMA
    bf16 = jnp.bfloat16
    swap = pltpu.VMEM((groups, blocks * parts, 128, wide), bf16)
    swap_far = pltpu.VMEM((groups - 1, blocks * parts, 128, wide), bf16)
    return pl.pallas_call(
        functools.partial(kernel, dims),
        out_shape=jax.ShapeDtypeStruct((rows, quarter), bf16),
        in_specs=[hbm_space] * 4 + [pl.BlockSpec(memory_space=pltpu.SMEM)],
        out_specs=pl.BlockSpec(memory_space=pltpu.VMEM),
        scratch_shapes=[
            pltpu.VMEM(queries.shape, bf16),
            pltpu.VMEM(out_weight.shape, bf16),
            pltpu.VMEM((2 * kv_heads, tokens, HEAD_SIZE), bf16),
            pltpu.VMEM((n, 8, 128), jnp.int32),
            pltpu.VMEM((blocks, tokens, 128), bf16),
            pltpu.VMEM((128, 128), bf16),
            pltpu.VMEM((n - 3, heads * rows, rows), jnp.float32),
            pltpu.VMEM((2, heads * rows, 128), jnp.float32),
            pltpu.VMEM((heads * rows, 256), jnp.float32),
            swap, swap, swap_far, swap_far,
            dma((2 * kv_heads + 2,)),
            dma((2 * kv_heads + 1, n, 3)), dma((2 * kv_heads + 1, n)),
            *[dma((groups, blocks * parts))] * 4,
        ],
        compiler_params=pltpu.CompilerParams(
            collective_id=0, has_side_effects=True, vmem_limit_bytes=53 * 2**20),
    )(queries, keys, values, out_weight, block_order)


def solution(mesh):
    n, tp = mesh.shape["ctx"], mesh.shape["tp"]
    in_specs = (P("ctx", "tp"), P("ctx", None), P("ctx", None), P("tp", None), P("ctx"))
    return jax.shard_map(functools.partial(shards, n, tp), mesh=mesh, in_specs=in_specs,
                         out_specs=P("ctx", "tp"), check_vma=False)
```

```python
import functools
import math

import jax
import jax.numpy as jnp
from jax import lax
from jax.experimental import pallas as pl
from jax.experimental.pallas import tpu as pltpu
from jax.sharding import PartitionSpec as P

QUERY_HEADS = 64
KEY_VALUE_HEADS = 8
HEAD_SIZE = 128
MESH = pl.DeviceIdType.MESH
NT = (((1,), (1,)), ((), ()))


ENDS = (
    (("own_across", 0, 1), ("keys", 1, 0), ("own_along", 0, 0), ("own_along", 0, 1), ("value", 1, 1), ("cross", 1, 1), ("own_across", 0, 0),),
    (),
    (),
    (("keys", 2, 0),),
    (),
    (("value", 2, 0), ("cross", 2, 0),),
    (("detour", 0, 0), ("value", 2, 1),),
    (("keys", 3, 0),),
    (("cross", 2, 1),),
    (("value", 1, 0),),
    (("value", 3, 0), ("cross", 1, 0), ("cross", 3, 0),),
    (("value", 3, 1), ("cross", 3, 1),),
    (),
    (),
    (),
)
INNER = (
    (("own_across", 0, 0), ("own_along", 0, 0), ("own_along", 0, 1), ("keys", 1, 0), ("own_across", 0, 1), ("keys", 2, 0),),
    (("value", 2, 0), ("value", 1, 0), ("value", 2, 1), ("value", 1, 1),),
    (),
    (("cross", 1, 1), ("cross", 1, 0), ("keys", 3, 0),),
    (("detour", 0, 0),),
    (("value", 3, 0), ("cross", 2, 1),),
    (),
    (("value", 3, 1), ("cross", 2, 0),),
    (("cross", 3, 1),),
    (),
    (),
    (("cross", 3, 0),),
    (),
    (),
    (),
)
DETOUR = (0, )


def kernel(dims, q_hbm, k_hbm, v_hbm, w_hbm, order_hbm, o_ref, order, q, w, kv, orders, mask, eye, scores,
           top, acc, pair_out, pair_in, far_out, far_in, load_sem, send, recv,
           pair_send, pair_recv, far_send, far_recv):
    n, tp, rows, heads, kv_heads, wide = dims
    line, groups = n // 2, tp // 2
    blocks = rows // 128
    per_kv = heads // kv_heads
    tile = per_kv * 128
    me, t = lax.axis_index("ctx"), lax.axis_index("tp")
    a, b = me // 2, lax.rem(me, 2)
    y, c = t // 2, lax.rem(t, 2)
    other = 1 - b
    partner = (me, y * 2 + 1 - c)

    def far(i):
        return lax.rem(y + i, groups)

    def guarded(cond, act):
        pl.when(cond)(act)

    up, down, across = a + 1 < line, a > 0, a * 2 + other

    barrier = pltpu.get_barrier_semaphore()

    def greet(target):
        pl.semaphore_signal(barrier, inc=1, device_id=target, device_id_type=MESH)

    guarded(up, lambda: greet((me + 2, t)))
    guarded(down, lambda: greet((me - 2, t)))
    greet((across, t))
    greet(partner)
    for i in range(1, groups):
        greet((me, far(i) * 2 + c))
    first = t * heads // (QUERY_HEADS // KEY_VALUE_HEADS)
    own = pl.ds(pl.multiple_of(me * rows, 128), rows)
    key_parts = range(0, 2 * kv_heads, 2)
    value_parts = range(1, 2 * kv_heads, 2)
    loads = {}
    for p in (*key_parts, *value_parts):
        src = v_hbm if p % 2 else k_hbm
        cols = pl.ds(pl.multiple_of((first + p // 2) * HEAD_SIZE, 128), HEAD_SIZE)
        loads[p] = pltpu.make_async_copy(src.at[:, cols], kv.at[p, own, :], load_sem.at[p])
        loads[p].start()
    q_load = pltpu.make_async_copy(q_hbm, q, load_sem.at[2 * kv_heads])
    w_load = pltpu.make_async_copy(w_hbm, w, load_sem.at[2 * kv_heads + 1])
    order_load = pltpu.make_async_copy(order_hbm, order, load_sem.at[2 * kv_heads + 2])
    order_load.start()

    pl.semaphore_wait(barrier, 1 + groups + up.astype(jnp.int32) + down.astype(jnp.int32))

    marks = 2 * kv_heads

    def piece(p, block, way, target):
        at = pl.ds(pl.multiple_of(block * rows, 128), rows)
        ref = orders.at[block] if p == marks else kv.at[p, at, :]
        return pltpu.make_async_remote_copy(
            src_ref=ref, dst_ref=ref, send_sem=send.at[p, block, way],
            recv_sem=recv.at[p, block], device_id=(target, t), device_id_type=MESH)

    def send_up(p, block):
        piece(p, block, 0, me + 2).start()

    def send_down(p, block):
        piece(p, block, 1, me - 2).start()

    def send_across(p, block):
        piece(p, block, 2, across).start()

    def arrived(p, block):
        piece(p, block, 2, me).wait_recv()

    def column(i):
        near = jnp.minimum(a, line - 1 - a)
        s = (i + 1) // 2
        zigzag = jnp.where(lax.rem(i, 2) == 1, a - s, a + s)
        onward = jnp.where(a < line - 1 - a, i, line - 1 - i)
        return jnp.where(i <= 2 * near, zigzag, onward)

    def onward(p, block):
        z = block // 2
        guarded(jnp.logical_and(up, z <= a), lambda: send_up(p, block))
        guarded(jnp.logical_and(down, z >= a), lambda: send_down(p, block))

    def near(i):
        return column(i) * 2 + b

    def crossed(i):
        return column(i) * 2 + other

    row = lax.broadcasted_iota(jnp.int32, (128, 128), 0)
    col = lax.broadcasted_iota(jnp.int32, (128, 128), 1)

    def build(i):
        for j in range(blocks):
            kpos = orders[pl.ds(i, 1), j:j + 1, :][0] * 128 + row
            for g in range(blocks):
                qpos = orders[pl.ds(me, 1), g:g + 1, :][0] * 128 + col
                at = pl.ds(pl.multiple_of(i * rows + j * 128, 128), 128)
                mask[g, at, :] = jnp.where(kpos <= qpos, 0.0, -1e30).astype(jnp.bfloat16)

    def launch(p):
        onward(p, me)
        send_across(p, me)

    for p in key_parts:
        loads[p].wait()
        launch(p)
    order_load.wait()
    for i in range(blocks):
        orders[pl.ds(me, 1), i:i + 1, :] = jnp.full((1, 1, 128), order[i], jnp.int32)
    launch(marks)
    q_load.start()
    for p in value_parts:
        loads[p].wait()
    w_load.start()
    eye[...] = (row == col).astype(jnp.bfloat16)
    q_load.wait()

    factor = math.log2(math.e) / math.sqrt(HEAD_SIZE)

    half = line // 2

    last = line - 1

    def near_slot(i):
        return 2 * i if i < last else 0

    def crossed_slot(i):
        return 2 * i + 1 if i < last - 1 else i - last + 2

    def span(h, g):
        return slice((h * blocks + g) * tile, (h * blocks + g + 1) * tile)

    def score(place, block, side, fresh=False):
        at = pl.ds(pl.multiple_of(block * rows, 128), rows)
        e = eye[...]
        for h in range(kv_heads):
            for g in range(blocks):
                ka = jnp.concatenate([kv[2 * h, at, :], mask[g, at, :]], axis=1)
                qa = jnp.concatenate(
                    [jnp.concatenate([q[g * 128:(g + 1) * 128, m * 128:(m + 1) * 128], e], axis=1)
                     for m in range(h * per_kv, (h + 1) * per_kv)], axis=0)
                s = lax.dot_general(qa, ka, NT, preferred_element_type=jnp.float32) * factor
                to = span(h, g)
                scores[place, to, :] = s
                best = None if fresh else top[side, to, :]
                for j in range(0, rows, 128):
                    best = s[:, j:j + 128] if best is None else jnp.maximum(best, s[:, j:j + 128])
                top[side, to, :] = best

    def score_near(i):
        build(near(i))
        score(near_slot(i), near(i), i // half, i % half == 0)

    def score_crossed(i):
        for p in (marks, *key_parts):
            arrived(p, crossed(i))
        build(crossed(i))
        score(crossed_slot(i), crossed(i), i // half)

    twin = a + 1 - 2 * lax.rem(a, 2)
    detour = DETOUR if line == 4 else ()

    def keys(i, _):
        for p in (marks, *key_parts):
            arrived(p, near(i))
            onward(p, near(i))
            send_across(p, near(i))

    def value(i, h):
        arrived(value_parts[h], near(i))
        onward(value_parts[h], near(i))

    def cross(i, h):
        if h in detour:
            guarded(column(i) != twin, lambda: send_across(value_parts[h], near(i)))
        else:
            send_across(value_parts[h], near(i))

    def detoured(h):
        block = a * 2 + other
        return (piece(value_parts[h], block, 0, me + 2), piece(value_parts[h], block, 1, me - 2))

    def detour_value(_, h):
        arrived(value_parts[h], a * 2 + other)
        rise, fall = detoured(h)
        guarded(twin > a, lambda: rise.start())
        guarded(twin < a, lambda: fall.start())

    def own_across(_, h):
        send_across(value_parts[h], me)

    def own_along(_, h):
        onward(value_parts[h], me)

    acts = dict(keys=keys, value=value, cross=cross, detour=detour_value,
                own_across=own_across, own_along=own_along)

    def issue(orders_of_work):
        for name, i, h in orders_of_work:
            acts[name](i, h)

    def take_values(i):
        for h, p in enumerate(value_parts):
            if i or h not in detour:
                arrived(p, crossed(i))

    def peak(side, at):
        return jnp.broadcast_to(jnp.max(top[side, at, :], axis=1, keepdims=True), (tile, 128))

    def settle_first():
        def body(i, _):
            at = pl.ds(pl.multiple_of(i * tile, 128), tile)
            top[0, at, :] = peak(0, at)
            return 0
        lax.fori_loop(0, kv_heads * blocks, body, 0)

    def settle_second():
        def body(i, _):
            at = pl.ds(pl.multiple_of(i * tile, 128), tile)
            before = top[0, at, :]
            after = jnp.maximum(before, peak(1, at))
            top[1, at, :] = after
            shrink = jnp.exp2(before - after)
            acc[at, :] = acc[at, :] * jnp.concatenate([shrink, shrink], axis=1)
            return 0
        lax.fori_loop(0, kv_heads * blocks, body, 0)

    def summed(h, g, pieces, side):
        to = span(h, g)
        best = top[side, to, :]
        weight = jnp.concatenate(
            [jnp.exp2(scores[place, to, j:j + 128] - best).astype(jnp.bfloat16)
             for place, _ in pieces for j in range(0, rows, 128)], axis=1)
        va = jnp.concatenate([kv[2 * h + 1, pl.ds(pl.multiple_of(block * rows, 128), rows), :]
                              for _, block in pieces], axis=0)
        va = jnp.concatenate([va, jnp.ones(va.shape, jnp.bfloat16)], axis=1)
        return jnp.dot(weight, va, preferred_element_type=jnp.float32)

    def absorb(pieces, side, fresh=False):
        for h in range(kv_heads):
            for g in range(blocks):
                part = summed(h, g, pieces, side)
                acc[span(h, g), :] = part if fresh else acc[span(h, g), :] + part

    def absorb_pair(i):
        take_values(i)
        absorb([(near_slot(i), near(i)), (crossed_slot(i), crossed(i))], i // half, i == 0)

    heads_of = range(kv_heads)
    every = {i: [("value", i, h) for h in heads_of] for i in range(line)}
    over = {i: [("cross", i, h) for h in heads_of] for i in range(line)}
    work = [([("own_across", 0, 0), *[("own_along", 0, h) for h in heads_of]], score_near, 0),
            ([("keys", 1, 0), *[("own_across", 0, h) for h in heads_of[1:]]], score_near, 1)]
    for i in range(2, last):
        if i == 2:
            work.append(([("keys", 2, 0)], score_crossed, 0))
        work.append(((every[1] if i == 2 else [("keys", i, 0)]) + over[i - 1] + every[i],
                     score_near, i))
        work.append(([], score_crossed, i - 1))
    work.append(([("keys", last, 0)], lambda _: settle_first(), 0))
    work.append((over[last - 1], absorb_pair, 0))
    work += [([], absorb_pair, i) for i in range(1, half - 1)]
    work.append(([], score_near, last))
    work.append((every[last], score_crossed, last - 1))
    work.append((over[last], absorb_pair, half - 1))
    work.append(([], score_crossed, last))
    work.append(([], lambda _: settle_second(), 0))
    work += [([], absorb_pair, i) for i in range(half, last)]
    work.append(([], lambda _: absorb([(near_slot(last), near(last))], 1), 0))

    at_end = jnp.logical_or(a == 0, a == last)
    for s, (common, act, i) in enumerate(work):
        if line == 4:
            if ENDS[s] == INNER[s]:
                issue(ENDS[s])
            else:
                guarded(at_end, lambda: issue(ENDS[s]))
                guarded(jnp.logical_not(at_end), lambda: issue(INNER[s]))
        else:
            issue(common)
        act(i)

    att = q

    def finish(g):
        for h in range(kv_heads):
            whole = acc[span(h, g), :] + summed(h, g, [(crossed_slot(last), crossed(last))], 1)
            res = (whole[:, :128] / whole[:, 128:]).astype(jnp.bfloat16)
            for m in range(per_kv):
                cols = (h * per_kv + m) * 128
                att[g * 128:(g + 1) * 128, cols:cols + 128] = res[m * 128:(m + 1) * 128]

    quarter = o_ref.shape[1]
    parts = quarter // wide

    def product(g, group, core, j):
        cols = pl.ds(pl.multiple_of((group * 2 + core) * quarter + j * wide, 128), wide)
        at = pl.ds(pl.multiple_of(g * 128, 128), 128)
        return jnp.dot(att[at, :], w[:, cols], preferred_element_type=jnp.float32)

    def pair_copy(i, k):
        return pltpu.make_async_remote_copy(
            src_ref=pair_out.at[i, k], dst_ref=pair_in.at[i, k], send_sem=pair_send.at[i, k],
            recv_sem=pair_recv.at[i, k], device_id=partner, device_id_type=MESH)

    def far_copy(i, k):
        return pltpu.make_async_remote_copy(
            src_ref=far_out.at[i - 1, k], dst_ref=far_in.at[i - 1, k], send_sem=far_send.at[i, k],
            recv_sem=far_recv.at[i, k], device_id=(me, far(i) * 2 + c), device_id_type=MESH)

    def lend(g, i, j):
        k = g * parts + j
        pair_out[i, k] = product(g, far(i), 1 - c, j).astype(jnp.bfloat16)
        pair_copy(i, k).start()

    def ship(g, i, j):
        k = g * parts + j
        mine = product(g, far(i), c, j)
        pair_copy(i, k).wait_recv()
        far_out[i - 1, k] = (mine + pair_in[i, k].astype(jnp.float32)).astype(jnp.bfloat16)
        far_copy(i, k).start()

    take_values(last)
    trips = [(g, i, j) for g in range(blocks) for i in range(1, groups) for j in range(parts)]
    ahead = 3
    for s, trip in enumerate(trips):
        if s % (len(trips) // blocks) == 0:
            finish(trip[0])
        if s == 0:
            w_load.wait()
        lend(*trip)
        if s >= ahead:
            ship(*trips[s - ahead])
    for trip in trips[-ahead:]:
        ship(*trip)

    def spot(k):
        return pl.ds(pl.multiple_of(k * 128, 128), 128)

    def near_step(k, _):
        g, j = k // parts, lax.rem(k, parts)
        lend(g, 0, j)
        acc[spot(k), :wide] = product(g, y, c, j)
        return 0
    lax.fori_loop(0, blocks * parts, near_step, 0)

    def close_step(k, _):
        g, j = k // parts, lax.rem(k, parts)
        pair_copy(0, k).wait_recv()
        res = acc[spot(k), :wide] + pair_in[0, k].astype(jnp.float32)
        for i in range(1, groups):
            far_copy(i, k).wait_recv()
            res = res + far_in[i - 1, k].astype(jnp.float32)
        o_ref[pl.ds(pl.multiple_of(g * 128, 128), 128),
              pl.ds(pl.multiple_of(j * wide, 128), wide)] = res.astype(jnp.bfloat16)
        return 0
    lax.fori_loop(0, blocks * parts, close_step, 0)

    def drain(i, _):
        for p in range(2 * kv_heads + 1):
            blk = i * 2 + b
            guarded(jnp.logical_and(up, i <= a), lambda: piece(p, blk, 0, me + 2).wait_send())
            guarded(jnp.logical_and(down, i >= a), lambda: piece(p, blk, 1, me - 2).wait_send())
            if p % 2 and p // 2 in detour:
                guarded(i != twin, lambda: piece(p, blk, 2, across).wait_send())
            else:
                piece(p, blk, 2, across).wait_send()
        return 0
    lax.fori_loop(0, line, drain, 0)
    for h in detour:
        rise, fall = detoured(h)
        guarded(twin > a, lambda: rise.wait_send())
        guarded(twin < a, lambda: fall.wait_send())

    def drain_out(j, _):
        for i in range(groups):
            pair_copy(i, j).wait_send()
            if i:
                far_copy(i, j).wait_send()
        return 0
    lax.fori_loop(0, blocks * parts, drain_out, 0)


def shards(n, tp, queries, keys, values, out_weight, block_order):
    rows = queries.shape[0]
    heads = queries.shape[1] // HEAD_SIZE
    group = QUERY_HEADS // KEY_VALUE_HEADS
    kv_heads = max(1, heads // group)
    quarter = out_weight.shape[1] // tp
    wide = min(256, quarter)
    parts, groups, tokens, blocks = quarter // wide, tp // 2, n * rows, rows // 128
    dims = (n, tp, rows, heads, kv_heads, wide)
    hbm_space = pl.BlockSpec(memory_space=pltpu.HBM)
    dma = pltpu.SemaphoreType.DMA
    bf16 = jnp.bfloat16
    swap = pltpu.VMEM((groups, blocks * parts, 128, wide), bf16)
    swap_far = pltpu.VMEM((groups - 1, blocks * parts, 128, wide), bf16)
    return pl.pallas_call(
        functools.partial(kernel, dims),
        out_shape=jax.ShapeDtypeStruct((rows, quarter), bf16),
        in_specs=[hbm_space] * 5,
        out_specs=pl.BlockSpec(memory_space=pltpu.VMEM),
        scratch_shapes=[
            pltpu.SMEM(block_order.shape, jnp.int32),
            pltpu.VMEM(queries.shape, bf16),
            pltpu.VMEM(out_weight.shape, bf16),
            pltpu.VMEM((2 * kv_heads, tokens, HEAD_SIZE), bf16),
            pltpu.VMEM((n, 8, 128), jnp.int32),
            pltpu.VMEM((blocks, tokens, 128), bf16),
            pltpu.VMEM((128, 128), bf16),
            pltpu.VMEM((n - 3, heads * rows, rows), jnp.float32),
            pltpu.VMEM((2, heads * rows, 128), jnp.float32),
            pltpu.VMEM((heads * rows, 256), jnp.float32),
            swap, swap, swap_far, swap_far,
            dma((2 * kv_heads + 3,)),
            dma((2 * kv_heads + 1, n, 3)), dma((2 * kv_heads + 1, n)),
            *[dma((groups, blocks * parts))] * 4,
        ],
        compiler_params=pltpu.CompilerParams(
            collective_id=0, has_side_effects=True, vmem_limit_bytes=53 * 2**20),
    )(queries, keys, values, out_weight, block_order)


def solution(mesh):
    n, tp = mesh.shape["ctx"], mesh.shape["tp"]
    in_specs = (P("ctx", "tp"), P("ctx", None), P("ctx", None), P("tp", None), P("ctx"))
    return jax.shard_map(functools.partial(shards, n, tp), mesh=mesh, in_specs=in_specs,
                         out_specs=P("ctx", "tp"), check_vma=False)
```

```python
import functools
import math

import jax
import jax.numpy as jnp
from jax import lax
from jax.experimental import pallas as pl
from jax.experimental.pallas import tpu as pltpu
from jax.sharding import PartitionSpec as P

QUERY_HEADS = 64
KEY_VALUE_HEADS = 8
HEAD_SIZE = 128
MESH = pl.DeviceIdType.MESH
NT = (((1,), (1,)), ((), ()))


ENDS = (
    (("own_across", 0, 1), ("keys", 1, 0), ("own_along", 0, 0), ("own_along", 0, 1), ("value", 1, 1), ("cross", 1, 1), ("own_across", 0, 0),),
    (),
    (),
    (("keys", 2, 0),),
    (),
    (("value", 2, 0), ("cross", 2, 0),),
    (("detour", 0, 0), ("value", 2, 1),),
    (("keys", 3, 0),),
    (("cross", 2, 1),),
    (("value", 1, 0),),
    (("value", 3, 0), ("cross", 1, 0), ("cross", 3, 0),),
    (("value", 3, 1), ("cross", 3, 1),),
    (),
    (),
    (),
)
INNER = (
    (("own_across", 0, 0), ("own_along", 0, 0), ("own_along", 0, 1), ("keys", 1, 0), ("own_across", 0, 1), ("keys", 2, 0),),
    (("value", 2, 0), ("value", 1, 0), ("value", 2, 1), ("value", 1, 1),),
    (),
    (("cross", 1, 1), ("cross", 1, 0), ("keys", 3, 0),),
    (("detour", 0, 0),),
    (("value", 3, 0), ("cross", 2, 1),),
    (),
    (("value", 3, 1), ("cross", 2, 0),),
    (("cross", 3, 1),),
    (),
    (),
    (("cross", 3, 0),),
    (),
    (),
    (),
)
DETOUR = (0, )


def kernel(dims, q_hbm, k_hbm, v_hbm, w_hbm, order_hbm, o_ref, order, q, w, kv, orders, mask, eye, scores,
           top, acc, pair_out, pair_in, far_out, far_in, load_sem, send, recv,
           pair_send, pair_recv, far_send, far_recv):
    n, tp, rows, heads, kv_heads, wide = dims
    line, groups = n // 2, tp // 2
    blocks = rows // 128
    per_kv = heads // kv_heads
    tile = per_kv * 128
    me, t = lax.axis_index("ctx"), lax.axis_index("tp")
    a, b = me // 2, lax.rem(me, 2)
    y, c = t // 2, lax.rem(t, 2)
    other = 1 - b
    partner = (me, y * 2 + 1 - c)

    def far(i):
        return lax.rem(y + i, groups)

    def guarded(cond, act):
        pl.when(cond)(act)

    up, down, across = a + 1 < line, a > 0, a * 2 + other

    barrier = pltpu.get_barrier_semaphore()

    def greet(target):
        pl.semaphore_signal(barrier, inc=1, device_id=target, device_id_type=MESH)

    guarded(up, lambda: greet((me + 2, t)))
    guarded(down, lambda: greet((me - 2, t)))
    greet((across, t))
    greet(partner)
    for i in range(1, groups):
        greet((me, far(i) * 2 + c))
    first = t * heads // (QUERY_HEADS // KEY_VALUE_HEADS)
    own = pl.ds(pl.multiple_of(me * rows, 128), rows)
    key_parts = range(0, 2 * kv_heads, 2)
    value_parts = range(1, 2 * kv_heads, 2)
    loads = {}
    for p in (*key_parts, *value_parts):
        src = v_hbm if p % 2 else k_hbm
        cols = pl.ds(pl.multiple_of((first + p // 2) * HEAD_SIZE, 128), HEAD_SIZE)
        loads[p] = pltpu.make_async_copy(src.at[:, cols], kv.at[p, own, :], load_sem.at[p])
        loads[p].start()
    q_load = pltpu.make_async_copy(q_hbm, q, load_sem.at[2 * kv_heads])
    w_load = pltpu.make_async_copy(w_hbm, w, load_sem.at[2 * kv_heads + 1])
    order_load = pltpu.make_async_copy(order_hbm, order, load_sem.at[2 * kv_heads + 2])
    order_load.start()

    pl.semaphore_wait(barrier, 1 + groups + up.astype(jnp.int32) + down.astype(jnp.int32))

    marks = 2 * kv_heads

    def piece(p, block, way, target):
        at = pl.ds(pl.multiple_of(block * rows, 128), rows)
        ref = orders.at[block] if p == marks else kv.at[p, at, :]
        return pltpu.make_async_remote_copy(
            src_ref=ref, dst_ref=ref, send_sem=send.at[p, block, way],
            recv_sem=recv.at[p, block], device_id=(target, t), device_id_type=MESH)

    def send_up(p, block):
        piece(p, block, 0, me + 2).start()

    def send_down(p, block):
        piece(p, block, 1, me - 2).start()

    def send_across(p, block):
        piece(p, block, 2, across).start()

    def arrived(p, block):
        piece(p, block, 2, me).wait_recv()

    def column(i):
        near = jnp.minimum(a, line - 1 - a)
        s = (i + 1) // 2
        zigzag = jnp.where(lax.rem(i, 2) == 1, a - s, a + s)
        onward = jnp.where(a < line - 1 - a, i, line - 1 - i)
        return jnp.where(i <= 2 * near, zigzag, onward)

    def onward(p, block):
        z = block // 2
        guarded(jnp.logical_and(up, z <= a), lambda: send_up(p, block))
        guarded(jnp.logical_and(down, z >= a), lambda: send_down(p, block))

    def near(i):
        return column(i) * 2 + b

    def crossed(i):
        return column(i) * 2 + other

    row = lax.broadcasted_iota(jnp.int32, (128, 128), 0)
    col = lax.broadcasted_iota(jnp.int32, (128, 128), 1)

    def build(i):
        for j in range(blocks):
            kpos = orders[pl.ds(i, 1), j:j + 1, :][0] * 128 + row
            for g in range(blocks):
                qpos = orders[pl.ds(me, 1), g:g + 1, :][0] * 128 + col
                at = pl.ds(pl.multiple_of(i * rows + j * 128, 128), 128)
                mask[g, at, :] = jnp.where(kpos <= qpos, 0.0, -1e30).astype(jnp.bfloat16)

    def launch(p):
        send_across(p, me)
        onward(p, me)

    for p in key_parts:
        loads[p].wait()
        launch(p)
    order_load.wait()
    for i in range(blocks):
        orders[pl.ds(me, 1), i:i + 1, :] = jnp.full((1, 1, 128), order[i], jnp.int32)
    launch(marks)
    q_load.start()
    for p in value_parts:
        loads[p].wait()
    w_load.start()
    eye[...] = (row == col).astype(jnp.bfloat16)
    q_load.wait()

    factor = math.log2(math.e) / math.sqrt(HEAD_SIZE)

    half = line // 2

    last = line - 1

    def near_slot(i):
        return 2 * i if i < last else 0

    def crossed_slot(i):
        return 2 * i + 1 if i < last - 1 else i - last + 2

    def span(h, g):
        return slice((h * blocks + g) * tile, (h * blocks + g + 1) * tile)

    def score(place, block, side, fresh=False):
        at = pl.ds(pl.multiple_of(block * rows, 128), rows)
        e = eye[...]
        for h in range(kv_heads):
            for g in range(blocks):
                ka = jnp.concatenate([kv[2 * h, at, :], mask[g, at, :]], axis=1)
                qa = jnp.concatenate(
                    [jnp.concatenate([q[g * 128:(g + 1) * 128, m * 128:(m + 1) * 128], e], axis=1)
                     for m in range(h * per_kv, (h + 1) * per_kv)], axis=0)
                s = lax.dot_general(qa, ka, NT, preferred_element_type=jnp.float32) * factor
                to = span(h, g)
                scores[place, to, :] = s
                best = None if fresh else top[side, to, :]
                for j in range(0, rows, 128):
                    best = s[:, j:j + 128] if best is None else jnp.maximum(best, s[:, j:j + 128])
                top[side, to, :] = best

    def score_near(i):
        build(near(i))
        score(near_slot(i), near(i), i // half, i % half == 0)

    def score_crossed(i):
        for p in (marks, *key_parts):
            arrived(p, crossed(i))
        build(crossed(i))
        score(crossed_slot(i), crossed(i), i // half)

    twin = a + 1 - 2 * lax.rem(a, 2)
    detour = DETOUR if line == 4 else ()

    def keys(i, _):
        for p in (*key_parts, marks):
            arrived(p, near(i))
            send_across(p, near(i))
            onward(p, near(i))

    def value(i, h):
        arrived(value_parts[h], near(i))
        onward(value_parts[h], near(i))

    def cross(i, h):
        if h in detour:
            guarded(column(i) != twin, lambda: send_across(value_parts[h], near(i)))
        else:
            send_across(value_parts[h], near(i))

    def detoured(h):
        block = a * 2 + other
        return (piece(value_parts[h], block, 0, me + 2), piece(value_parts[h], block, 1, me - 2))

    def detour_value(_, h):
        arrived(value_parts[h], a * 2 + other)
        rise, fall = detoured(h)
        guarded(twin > a, lambda: rise.start())
        guarded(twin < a, lambda: fall.start())

    def own_across(_, h):
        send_across(value_parts[h], me)

    def own_along(_, h):
        onward(value_parts[h], me)

    acts = dict(keys=keys, value=value, cross=cross, detour=detour_value,
                own_across=own_across, own_along=own_along)

    def issue(orders_of_work):
        for name, i, h in orders_of_work:
            acts[name](i, h)

    def take_values(i):
        for h, p in enumerate(value_parts):
            if i or h not in detour:
                arrived(p, crossed(i))

    def peak(side, at):
        return jnp.broadcast_to(jnp.max(top[side, at, :], axis=1, keepdims=True), (tile, 128))

    def settle_first():
        def body(i, _):
            at = pl.ds(pl.multiple_of(i * tile, 128), tile)
            top[0, at, :] = peak(0, at)
            return 0
        lax.fori_loop(0, kv_heads * blocks, body, 0)

    def settle_second():
        def body(i, _):
            at = pl.ds(pl.multiple_of(i * tile, 128), tile)
            before = top[0, at, :]
            after = jnp.maximum(before, peak(1, at))
            top[1, at, :] = after
            shrink = jnp.exp2(before - after)
            acc[at, :] = acc[at, :] * jnp.concatenate([shrink, shrink], axis=1)
            return 0
        lax.fori_loop(0, kv_heads * blocks, body, 0)

    def summed(h, g, pieces, side):
        to = span(h, g)
        best = top[side, to, :]
        weight = jnp.concatenate(
            [jnp.exp2(scores[place, to, j:j + 128] - best).astype(jnp.bfloat16)
             for place, _ in pieces for j in range(0, rows, 128)], axis=1)
        va = jnp.concatenate([kv[2 * h + 1, pl.ds(pl.multiple_of(block * rows, 128), rows), :]
                              for _, block in pieces], axis=0)
        va = jnp.concatenate([va, jnp.ones(va.shape, jnp.bfloat16)], axis=1)
        return jnp.dot(weight, va, preferred_element_type=jnp.float32)

    def absorb(pieces, side, fresh=False):
        for h in range(kv_heads):
            for g in range(blocks):
                part = summed(h, g, pieces, side)
                acc[span(h, g), :] = part if fresh else acc[span(h, g), :] + part

    def absorb_pair(i):
        take_values(i)
        absorb([(near_slot(i), near(i)), (crossed_slot(i), crossed(i))], i // half, i == 0)

    heads_of = range(kv_heads)
    every = {i: [("value", i, h) for h in heads_of] for i in range(line)}
    over = {i: [("cross", i, h) for h in heads_of] for i in range(line)}
    work = [([("own_across", 0, 0), *[("own_along", 0, h) for h in heads_of]], score_near, 0),
            ([("keys", 1, 0), *[("own_across", 0, h) for h in heads_of[1:]]], score_near, 1)]
    for i in range(2, last):
        if i == 2:
            work.append(([("keys", 2, 0)], score_crossed, 0))
        work.append(((every[1] if i == 2 else [("keys", i, 0)]) + over[i - 1] + every[i],
                     score_near, i))
        work.append(([], score_crossed, i - 1))
    work.append(([("keys", last, 0)], lambda _: settle_first(), 0))
    work.append((over[last - 1], absorb_pair, 0))
    work += [([], absorb_pair, i) for i in range(1, half - 1)]
    work.append(([], score_near, last))
    work.append((every[last], score_crossed, last - 1))
    work.append((over[last], absorb_pair, half - 1))
    work.append(([], score_crossed, last))
    work.append(([], lambda _: settle_second(), 0))
    work += [([], absorb_pair, i) for i in range(half, last)]
    work.append(([], lambda _: absorb([(near_slot(last), near(last))], 1), 0))

    at_end = jnp.logical_or(a == 0, a == last)
    for s, (common, act, i) in enumerate(work):
        if line == 4:
            if ENDS[s] == INNER[s]:
                issue(ENDS[s])
            else:
                guarded(at_end, lambda: issue(ENDS[s]))
                guarded(jnp.logical_not(at_end), lambda: issue(INNER[s]))
        else:
            issue(common)
        act(i)

    att = q

    def finish(g):
        for h in range(kv_heads):
            whole = acc[span(h, g), :] + summed(h, g, [(crossed_slot(last), crossed(last))], 1)
            res = (whole[:, :128] / whole[:, 128:]).astype(jnp.bfloat16)
            for m in range(per_kv):
                cols = (h * per_kv + m) * 128
                att[g * 128:(g + 1) * 128, cols:cols + 128] = res[m * 128:(m + 1) * 128]

    quarter = o_ref.shape[1]
    parts = quarter // wide

    def product(g, group, core, j):
        cols = pl.ds(pl.multiple_of((group * 2 + core) * quarter + j * wide, 128), wide)
        at = pl.ds(pl.multiple_of(g * 128, 128), 128)
        return jnp.dot(att[at, :], w[:, cols], preferred_element_type=jnp.float32)

    def pair_copy(i, k):
        return pltpu.make_async_remote_copy(
            src_ref=pair_out.at[i, k], dst_ref=pair_in.at[i, k], send_sem=pair_send.at[i, k],
            recv_sem=pair_recv.at[i, k], device_id=partner, device_id_type=MESH)

    def far_copy(i, k):
        return pltpu.make_async_remote_copy(
            src_ref=far_out.at[i - 1, k], dst_ref=far_in.at[i - 1, k], send_sem=far_send.at[i, k],
            recv_sem=far_recv.at[i, k], device_id=(me, far(i) * 2 + c), device_id_type=MESH)

    def lend(g, i, j):
        k = g * parts + j
        pair_out[i, k] = product(g, far(i), 1 - c, j).astype(jnp.bfloat16)
        pair_copy(i, k).start()

    def ship(g, i, j):
        k = g * parts + j
        mine = product(g, far(i), c, j)
        pair_copy(i, k).wait_recv()
        far_out[i - 1, k] = (mine + pair_in[i, k].astype(jnp.float32)).astype(jnp.bfloat16)
        far_copy(i, k).start()

    take_values(last)
    trips = [(g, i, j) for g in range(blocks) for i in range(1, groups) for j in range(parts)]
    ahead = 3
    for s, trip in enumerate(trips):
        if s % (len(trips) // blocks) == 0:
            finish(trip[0])
        if s == 0:
            w_load.wait()
        lend(*trip)
        if s >= ahead:
            ship(*trips[s - ahead])
    for trip in trips[-ahead:]:
        ship(*trip)

    def spot(k):
        return pl.ds(pl.multiple_of(k * 128, 128), 128)

    def near_step(k, _):
        g, j = k // parts, lax.rem(k, parts)
        lend(g, 0, j)
        acc[spot(k), :wide] = product(g, y, c, j)
        return 0
    lax.fori_loop(0, blocks * parts, near_step, 0)

    def close_step(k, _):
        g, j = k // parts, lax.rem(k, parts)
        pair_copy(0, k).wait_recv()
        res = acc[spot(k), :wide] + pair_in[0, k].astype(jnp.float32)
        for i in range(1, groups):
            far_copy(i, k).wait_recv()
            res = res + far_in[i - 1, k].astype(jnp.float32)
        o_ref[pl.ds(pl.multiple_of(g * 128, 128), 128),
              pl.ds(pl.multiple_of(j * wide, 128), wide)] = res.astype(jnp.bfloat16)
        return 0
    lax.fori_loop(0, blocks * parts, close_step, 0)

    def drain(i, _):
        for p in range(2 * kv_heads + 1):
            blk = i * 2 + b
            guarded(jnp.logical_and(up, i <= a), lambda: piece(p, blk, 0, me + 2).wait_send())
            guarded(jnp.logical_and(down, i >= a), lambda: piece(p, blk, 1, me - 2).wait_send())
            if p % 2 and p // 2 in detour:
                guarded(i != twin, lambda: piece(p, blk, 2, across).wait_send())
            else:
                piece(p, blk, 2, across).wait_send()
        return 0
    lax.fori_loop(0, line, drain, 0)
    for h in detour:
        rise, fall = detoured(h)
        guarded(twin > a, lambda: rise.wait_send())
        guarded(twin < a, lambda: fall.wait_send())

    def drain_out(j, _):
        for i in range(groups):
            pair_copy(i, j).wait_send()
            if i:
                far_copy(i, j).wait_send()
        return 0
    lax.fori_loop(0, blocks * parts, drain_out, 0)


def shards(n, tp, queries, keys, values, out_weight, block_order):
    rows = queries.shape[0]
    heads = queries.shape[1] // HEAD_SIZE
    group = QUERY_HEADS // KEY_VALUE_HEADS
    kv_heads = max(1, heads // group)
    quarter = out_weight.shape[1] // tp
    wide = min(256, quarter)
    parts, groups, tokens, blocks = quarter // wide, tp // 2, n * rows, rows // 128
    dims = (n, tp, rows, heads, kv_heads, wide)
    hbm_space = pl.BlockSpec(memory_space=pltpu.HBM)
    dma = pltpu.SemaphoreType.DMA
    bf16 = jnp.bfloat16
    swap = pltpu.VMEM((groups, blocks * parts, 128, wide), bf16)
    swap_far = pltpu.VMEM((groups - 1, blocks * parts, 128, wide), bf16)
    return pl.pallas_call(
        functools.partial(kernel, dims),
        out_shape=jax.ShapeDtypeStruct((rows, quarter), bf16),
        in_specs=[hbm_space] * 5,
        out_specs=pl.BlockSpec(memory_space=pltpu.VMEM),
        scratch_shapes=[
            pltpu.SMEM(block_order.shape, jnp.int32),
            pltpu.VMEM(queries.shape, bf16),
            pltpu.VMEM(out_weight.shape, bf16),
            pltpu.VMEM((2 * kv_heads, tokens, HEAD_SIZE), bf16),
            pltpu.VMEM((n, 8, 128), jnp.int32),
            pltpu.VMEM((blocks, tokens, 128), bf16),
            pltpu.VMEM((128, 128), bf16),
            pltpu.VMEM((n - 3, heads * rows, rows), jnp.float32),
            pltpu.VMEM((2, heads * rows, 128), jnp.float32),
            pltpu.VMEM((heads * rows, 256), jnp.float32),
            swap, swap, swap_far, swap_far,
            dma((2 * kv_heads + 3,)),
            dma((2 * kv_heads + 1, n, 3)), dma((2 * kv_heads + 1, n)),
            *[dma((groups, blocks * parts))] * 4,
        ],
        compiler_params=pltpu.CompilerParams(
            collective_id=0, has_side_effects=True, vmem_limit_bytes=53 * 2**20),
    )(queries, keys, values, out_weight, block_order)


def solution(mesh):
    n, tp = mesh.shape["ctx"], mesh.shape["tp"]
    in_specs = (P("ctx", "tp"), P("ctx", None), P("ctx", None), P("tp", None), P("ctx"))
    return jax.shard_map(functools.partial(shards, n, tp), mesh=mesh, in_specs=in_specs,
                         out_specs=P("ctx", "tp"), check_vma=False)
```
